256 devices in a mesh: dp: 32 (over y, z), vocab: 8 (over x, core).
Axes of the slice: x: 4, y: 4, z: 8, core: 2. Of those that a mesh axis runs over, the one named last changes fastest.
Arguments:
- hidden_states: bfloat16 [16384, 2048], P('dp', 'vocab'), may hold values from -12 to 12
- teacher_logits: bfloat16 [16384, 16384], P('dp', 'vocab'), may hold values from -24 to 240
- head_weight: bfloat16 [2048, 16384], P(None, 'vocab'), as said below
Outputs:
- kl_per_token: float32 [16384], P('dp')
- hidden_grad: bfloat16 [16384, 2048], P('dp', 'vocab')
- head_grad: float32 [2048, 16384], P('dp', 'vocab')
The draws below stay inside these ranges and needn't reach their ends.
Inputs may be any that keep to these rules, and one draw needn't show every extreme that they name: `head_weight`: every entry's magnitude is at most 18 / sqrt(2048).
All inputs are finite; a program needn't handle non-finite values.
Results may differ from the reference program's by a relative error of at most 0.014.
Values may be sent and summed in bfloat16 or wider, within the bound.
No kernel may reach another device: no remote copies, remote signals or barrier semaphores. Data moves between devices by JAX's collectives and lax.ppermute only.
A program may use at most 128 MiB of HBM per device.

```python
import math
import jax
import jax.numpy as jnp
from jax import lax

D = 2048
V = 16384
MICRO = 2
TOK = 256
TOKENS = 16384
N_DP = 32


def head_columns(key):
    column_key = jax.random.fold_in(key, 7101)
    value_key = jax.random.fold_in(column_key, 1)
    spread = 3.0 / math.sqrt(D)
    values = jnp.clip(jax.random.normal(value_key, (D, V), jnp.float32), -6.0, 6.0)
    return values * spread


def draw_head_weight(key, part):
    return head_columns(key).astype(jnp.bfloat16)


def draw_hidden_states(key, part):
    streams = jax.random.split(jax.random.fold_in(key, 7202), 2)
    values = jnp.clip(jax.random.normal(streams[1], (TOKENS, D), jnp.float32), -6.0, 6.0)
    return values.astype(jnp.bfloat16)


def draw_teacher_logits(key, part):
    streams = jax.random.split(jax.random.fold_in(key, 7303), 3)
    values = 3.0 * jnp.clip(jax.random.normal(streams[2], (TOKENS, V), jnp.float32), -8.0, 8.0)
    return values.astype(jnp.bfloat16)


def setup_inputs(seed: int = 0) -> dict:
    key_list = jax.random.split(jax.random.key(seed), 4)
    hidden_states = draw_hidden_states(jax.random.fold_in(key_list[3], 71), 0)
    teacher_logits = draw_teacher_logits(jax.random.fold_in(key_list[3], 71), 0)
    head_weight = draw_head_weight(jax.random.fold_in(key_list[3], 71), 0)
    return {"hidden_states": hidden_states, "teacher_logits": teacher_logits, "head_weight": head_weight}


grad_scale = 8.0


def token_group(hidden_rows, teacher_rows, head_weight):
    student = jnp.dot(hidden_rows, head_weight, preferred_element_type=jnp.float32)
    teacher = teacher_rows.astype(jnp.float32)
    student_max = jnp.max(student, axis=1, keepdims=True)
    teacher_max = jnp.max(teacher, axis=1, keepdims=True)
    student_terms = jnp.exp(student - student_max)
    teacher_terms = jnp.exp(teacher - teacher_max)
    student_total = jnp.sum(student_terms, axis=1)
    teacher_total = jnp.sum(teacher_terms, axis=1)
    cross_term = jnp.sum(teacher_terms * (teacher - student), axis=1)
    divergence = cross_term / teacher_total - teacher_max[:, 0] - jnp.log(teacher_total) + student_max[:, 0] + jnp.log(student_total)
    logit_grad = (grad_scale * (student_terms / student_total[:, None] - teacher_terms / teacher_total[:, None])).astype(jnp.bfloat16)
    hidden_grad = lax.dot_general(logit_grad, head_weight, (((1,), (1,)), ((), ())), preferred_element_type=jnp.float32).astype(jnp.bfloat16)
    group_grad = lax.dot_general(hidden_rows, logit_grad, (((0,), (0,)), ((), ())), preferred_element_type=jnp.float32).astype(jnp.bfloat16)
    return divergence, hidden_grad, group_grad


def reference(hidden_states, teacher_logits, head_weight):
    group_rows = MICRO * TOK
    grouped_hidden = hidden_states.reshape(N_DP, group_rows, D)
    grouped_teacher = teacher_logits.reshape(N_DP, group_rows, V)

    def one_group(running, inputs):
        divergence, hidden_grad, group_grad = token_group(inputs[0], inputs[1], head_weight)
        running = running + lax.optimization_barrier(group_grad).astype(jnp.float32)
        return running, (divergence, hidden_grad)

    head_grad, results = lax.scan(one_group, jnp.zeros((D, V), jnp.float32), (grouped_hidden, grouped_teacher))
    divergence = results[0].reshape(TOKENS)
    hidden_grad = results[1].reshape(TOKENS, D)
    return divergence, hidden_grad, head_grad
```

```python
import functools

import jax
import jax.numpy as jnp
from jax import lax
from jax.experimental import pallas as pl
from jax.experimental.pallas import tpu as pltpu
from jax.sharding import Mesh
from jax.sharding import PartitionSpec as P


DP = ("y", "p", "q")
VOCAB = ("x", "c")
WHOLE_VOCAB = ("q", "x", "c")
SWAP = ((0, 1), (1, 0))
CHUNKS = (512, 512)


grad_scale = 8.0
BF = jnp.bfloat16
F32 = jnp.float32


def sent(array, axis, by):
    size = lax.axis_size(axis)
    return lax.ppermute(array, axis, [(k, (k + by) % size) for k in range(size)])


def swapped(array, axis):
    return lax.ppermute(array, axis, SWAP)


def sent_to_all(array, axis):
    copies = jnp.broadcast_to(array, (lax.axis_size(axis), *array.shape))
    return lax.all_to_all(copies, axis, 0, 0, tiled=True)


def whole(shape):
    return pl.BlockSpec(shape, lambda *_: (0,) * len(shape))


def after(array, *others):
    return lax.optimization_barrier((array, *others))[0]


def call(body, where, operands, in_specs, out_shapes, out_specs, grid=(1,), scratch=(), micros=2, vmem=20):
    operands = [
        pltpu.with_memory_space_constraint(array, pltpu.HBM) if array.size >= 2**17 else array
        for array in operands
    ]
    out_shapes = jax.tree.map(
        lambda s: pltpu.HBM(s.shape, s.dtype) if s.size >= 2**17 else s, out_shapes
    )
    cost = pl.CostEstimate(flops=int(micros * 4.5e8), bytes_accessed=2**20, transcendentals=0)
    return pl.pallas_call(
        body,
        cost_estimate=cost,
        out_shape=out_shapes,
        grid_spec=pltpu.PrefetchScalarGridSpec(
            num_scalar_prefetch=1,
            grid=grid,
            in_specs=in_specs,
            out_specs=out_specs,
            scratch_shapes=scratch,
        ),
        compiler_params=pltpu.CompilerParams(vmem_limit_bytes=vmem * 2**20),
    )(where, *operands)


def as_row(column):
    return jnp.transpose(jnp.broadcast_to(column, (column.shape[0], 128)))[0:1]


def lane_sums(value):
    lanes = value[:, 0:128]
    for k in range(128, value.shape[1], 128):
        lanes = lanes + value[:, k : k + 128]
    return jnp.sum(lanes, axis=1, keepdims=True)


def totals(stats, value, row_block=128):
    rows, columns = value.shape
    found = ([], [])
    for at in range(0, rows, row_block):
        part = value[at : at + row_block, :].astype(F32)
        lanes = part[:, 0:128]
        for k in range(128, columns, 128):
            lanes = jnp.maximum(lanes, part[:, k : k + 128])
        peak = jnp.max(lanes, axis=1, keepdims=True)
        found[0].append(peak)
        found[1].append(lane_sums(jnp.exp(part - peak)))
    for k, part in enumerate(found):
        stats[k : k + 1, :] = as_row(jnp.concatenate(part, axis=0))


def join_body(where, *refs):
    rows = refs[0].shape[0]
    for k, ref in enumerate(refs[:-1]):
        refs[-1][k * rows : (k + 1) * rows, :] = ref[...]


def student_body(block, where, mine, other, *refs):
    weights, (total, stats) = refs[:4], refs[4:]
    c = where[4]
    width = mine.shape[1]
    rows = mine.shape[0] // 4
    step = pl.program_id(0)
    value = None
    for k in range(4):
        for side, slices in enumerate((mine, other)):
            at = pl.multiple_of((c if side == 0 else 1 - c) * width, width)
            got = jnp.dot(
                slices[k * rows : (k + 1) * rows, :],
                weights[k][pl.ds(at, width), :],
                preferred_element_type=F32,
            )
            value = got if value is None else value + got
    total[:, pl.ds(pl.multiple_of(step * block, block), block)] = value

    @pl.when(step == pl.num_programs(0) - 1)
    def _():
        totals(stats, total)


def student_part(where, pair, weight, block=256):
    rows = pair[0].shape[0] // 4
    columns = weight.shape[1] // 2
    width = pair[0].shape[1]
    steps = columns // block
    in_specs = [whole(pair[0].shape)] * 2
    for by in range(4):
        in_specs.append(
            pl.BlockSpec(
                (2 * width, block),
                lambda j, at, by=by: (lax.rem(at[3] + by, 4), at[2] * steps + j),
            )
        )
    return call(
        functools.partial(student_body, block),
        where,
        [*pair, *[weight] * 4],
        in_specs,
        [jax.ShapeDtypeStruct((rows, columns), F32), jax.ShapeDtypeStruct((2, rows), F32)],
        [whole((rows, columns)), whole((2, rows))],
        (steps,),
        micros=8,
        vmem=28,
    )


def teacher_body(where, teacher, stats):
    totals(stats, teacher)


def arrange_body(where, *refs):
    pairs, outs = refs[:-4], refs[-4:]
    y, x, c = where[0], where[3], where[4]
    width = pairs[0].shape[1]
    rows = outs[0].shape[0] // 2
    for r in range(4):
        d = lax.rem(x + r - y + 4, 4)
        for side in range(4):

            @pl.when(d == side)
            def _(r=r, side=side):
                for group in range(2):
                    mine = pairs[2 * group][r * rows : (r + 1) * rows, :]
                    other = pairs[2 * group + 1][r * rows : (r + 1) * rows, :]
                    to = slice(group * rows, (group + 1) * rows)
                    outs[side][to, 0:width] = jnp.where(c == 0, mine, other)
                    outs[side][to, width : 2 * width] = jnp.where(c == 0, other, mine)


def merged(parts):
    top = jnp.max(parts[0][:, 0], axis=0, keepdims=True)
    for part in parts[1:]:
        top = jnp.maximum(top, jnp.max(part[:, 0], axis=0, keepdims=True))
    total = sum(
        jnp.sum(part[:, 1] * jnp.exp(part[:, 0] - top), axis=0, keepdims=True) for part in parts
    )
    return top, total


def grad_body(first, where, s_own, s_other, t_own, t_other, every_s, every_t, out, *refs):
    if first:
        scales = refs
    else:
        tops, cross, *scales = refs
    q = where[2]
    step = pl.program_id(0)
    steps = pl.num_programs(0)
    block = s_own.shape[0]
    rows = every_t.shape[2]
    half = every_s.shape[0] // 2

    @pl.when(step == 0)
    def _():
        for group in range(2):
            at = slice(group * rows, (group + 1) * rows)
            to = slice((1 - group) * rows, (2 - group) * rows)
            mine = every_s[pl.ds(q * half, half), :, at]
            other = every_s[pl.ds((1 - q) * half, half), :, to]
            s_top, s_total = merged((mine, other))
            source = q if group == 0 else 1 - q
            t_top, t_total = merged((every_t[pl.ds(source * half, half), :, :],))
            if group == 0 and not first:
                for k, row in enumerate((s_top, s_total, t_top, t_total)):
                    tops[k : k + 1, :] = row
            wanted = (s_top, grad_scale / s_total, t_top, grad_scale / t_total)
            for row, scale in zip(wanted, scales):
                scale[at, :] = jnp.transpose(jnp.broadcast_to(row, (128, rows)))

    def rows_of(student, teacher):
        at = pl.ds(pl.multiple_of(step * block, block), block)
        s_top, s_scale, t_top, t_scale = (scale[at, :] for scale in scales)
        begin = student.shape[1] - out.shape[1]
        lanes = None
        for k in range(0, student.shape[1], 128):
            s = student[:, k : k + 128]
            t = teacher[:, k : k + 128].astype(F32)
            t_term = jnp.exp(t - t_top)
            if k >= begin:
                out[:, k - begin : k - begin + 128] = (
                    jnp.exp(s - s_top) * s_scale - t_term * t_scale
                ).astype(BF)
            if not first:
                term = t_term * (t - s)
                lanes = term if lanes is None else lanes + term
        if not first:
            cross[0:1, at] = as_row(jnp.sum(lanes, axis=1, keepdims=True))

    @pl.when(step < steps // 2)
    def _():
        rows_of(s_own, t_own)

    @pl.when(step >= steps // 2)
    def _():
        rows_of(s_other, t_other)


def grad_part(where, values, every_s, every_t, count, first, block=256):
    rows, half = values[0].shape
    steps = 2 * rows // block
    read = count if first else half
    early = pl.BlockSpec((block, read), lambda j, at: (jnp.minimum(j, steps // 2 - 1), 0))
    late = pl.BlockSpec((block, read), lambda j, at: (jnp.maximum(j - steps // 2, 0), 0))
    shapes = [jax.ShapeDtypeStruct((2 * rows, count), BF)]
    specs = [pl.BlockSpec((block, count), lambda j, at: (j, 0))]
    if not first:
        more = ((4, rows), (1, 2 * rows))
        shapes += [jax.ShapeDtypeStruct(shape, F32) for shape in more]
        specs += [whole(shape) for shape in more]
    return call(
        functools.partial(grad_body, first),
        where,
        [*values, every_s, every_t],
        [early, late, early, late, whole(every_s.shape), whole(every_t.shape)],
        shapes,
        specs,
        (steps,),
        [pltpu.VMEM((2 * rows, 128), F32)] * 4,
        micros=4,
    )


def hidden_body(with_arrived, where, first, last, weight, *refs):
    split = first.shape[1]
    value = None
    for grad, columns in ((first, slice(0, split)), (last, slice(split, None))):
        part = lax.dot_general(
            grad[...], weight[:, columns], (((1,), (1,)), ((), ())), preferred_element_type=F32
        )
        value = part if value is None else value + part
    if with_arrived:
        value = value + refs[0][0].astype(F32)
    refs[-1][0] = value.astype(BF)


def hidden_part(where, grads, weight, this_core, arrived=None):
    tokens = grads[0].shape[0]
    half = weight.shape[1] // 2
    width = 256

    def block_of(j, at):
        core = at[4] if this_core else 1 - at[4]
        return (2 * lax.rem(at[3] + j, 4) + core, at[2])

    tile = pl.BlockSpec((1, tokens, width), lambda j, at: (j, 0, 0))
    operands = [*grads, weight]
    in_specs = [*(whole(grad.shape) for grad in grads), pl.BlockSpec((width, half), block_of)]
    if arrived is not None:
        operands.append(arrived)
        in_specs.append(tile)
    return call(
        functools.partial(hidden_body, arrived is not None),
        where,
        operands,
        in_specs,
        jax.ShapeDtypeStruct((4, tokens, width), BF),
        tile,
        (4,),
        micros=6,
    )


def final_body(where, *refs):
    out = refs[-1]
    half = out.shape[1] // 2
    begin = 0
    for piece in refs[:-1]:
        chunk = piece.shape[2]
        for side in (0, 1):
            at = side * half + begin
            out[:, at : at + chunk] = sum(piece[2 * p + side].astype(F32) for p in range(4))
        begin += chunk


def per_device(hidden_states, teacher_logits, head_weight):
    rows, width = hidden_states.shape
    _, columns = head_weight.shape
    half = columns // 2
    where = jnp.stack([lax.axis_index(name) for name in (*DP, *VOCAB)]).astype(jnp.int32)
    q = lax.axis_index("q")

    other_hidden = swapped(hidden_states, "q")
    (teacher_stats,) = call(
        teacher_body,
        where,
        [teacher_logits],
        [whole(teacher_logits.shape)],
        [jax.ShapeDtypeStruct((2, rows), F32)],
        [whole((2, rows))],
        micros=5,
    )
    every_teacher = sent_to_all(teacher_stats, WHOLE_VOCAB)
    pairs = []
    for piece in (hidden_states, other_hidden):
        moved = [sent(piece, "x", by) for by in (-1, 2, 1)]
        mine = call(
            join_body,
            where,
            [piece, *moved],
            [whole(piece.shape)] * 4,
            jax.ShapeDtypeStruct((4 * rows, width), BF),
            whole((4 * rows, width)),
            micros=1,
        )
        pairs.append((mine, swapped(mine, "c")))
    kept_teacher = lax.dynamic_slice_in_dim(teacher_logits, q * half, half, 1)
    later = after(teacher_logits, other_hidden)
    sent_teacher = lax.dynamic_slice_in_dim(later, (1 - q) * half, half, 1)
    arrived_teacher = swapped(sent_teacher, "q")

    student_own, stats_own = student_part(where, pairs[0], head_weight)
    student_other, stats_other = student_part(where, pairs[1], head_weight)
    every_student = sent_to_all(jnp.concatenate([stats_own, stats_other], axis=1), WHOLE_VOCAB)
    flat = [array for pair in pairs for array in pair]
    blocks = call(
        arrange_body,
        where,
        flat,
        [whole(array.shape) for array in flat],
        [jax.ShapeDtypeStruct((2 * rows, 2 * width), BF)] * 4,
        [whole((2 * rows, 2 * width))] * 4,
        micros=5,
    )
    values = (student_own, student_other, kept_teacher, arrived_teacher)
    (grad_first,) = grad_part(where, values, every_student, every_teacher, CHUNKS[0], True)

    pieces = []
    begin = -CHUNKS[0]
    grads = grad_first
    gate = None
    for k, chunk in enumerate(CHUNKS):
        if k:
            grads = after(grad_last, gate)[:, begin : begin + chunk]
        begin += chunk
        parts = []
        for d in (2, 1, 3):
            part = lax.dot_general(
                blocks[d], grads, (((0,), (0,)), ((), ())), preferred_element_type=F32
            ).astype(BF)
            parts.append(sent(part, "y", d))
        if k == 0:
            later = tuple(after(value, part) for value in values)
            grad_last, tops, cross = grad_part(
                where, later, every_student, every_teacher, half - CHUNKS[0], False
            )
            crosses = sent_to_all(cross, WHOLE_VOCAB)
            across_core = hidden_part(where, (grad_first, grad_last), head_weight, False)
            across_core = swapped(across_core, "c")
            gate = grad_last
        else:
            gate = part
        own = lax.dot_general(
            blocks[0], grads, (((0,), (0,)), ((), ())), preferred_element_type=F32
        )
        total = own + sum(part.astype(F32) for part in parts)
        total = total.astype(BF).reshape(8, -1, chunk)
        pieces.append(lax.all_to_all(total, ("p", "q"), 0, 0, tiled=True))
        if k == 0:
            value = hidden_part(
                where, (grad_first, after(grad_last, total)), head_weight, True, across_core
            )
    head_grad = call(
        final_body,
        where,
        pieces,
        [whole(piece.shape) for piece in pieces],
        jax.ShapeDtypeStruct((pieces[0].shape[1], columns), F32),
        whole((pieces[0].shape[1], columns)),
    )
    moved = [sent(value[d], "x", d) for d in (2, 1, 3)]
    value = value[0].astype(F32) + sum(part.astype(F32) for part in moved)
    partner = swapped(value[rows:].astype(BF), "q")
    hidden_grad = (value[:rows] + partner.astype(F32)).astype(BF)

    crosses = jnp.sum(crosses[:, 0].reshape(2, -1, 2, rows), axis=1)
    cross_term = jnp.where(q == 0, crosses[0, 0] + crosses[1, 1], crosses[1, 0] + crosses[0, 1])
    student_max, student_total, teacher_max, teacher_total = tops
    divergence = (
        cross_term / teacher_total
        - teacher_max
        - jnp.log(teacher_total)
        + student_max
        + jnp.log(student_total)
    )
    return divergence, hidden_grad, head_grad


def solution(mesh):
    split = Mesh(mesh.devices.reshape(4, 4, 2, 4, 2), (*DP, *VOCAB))
    placed = (P(DP, VOCAB), P(DP, VOCAB), P(None, VOCAB))

    return jax.shard_map(
        per_device,
        mesh=split,
        in_specs=placed,
        out_specs=(P(DP), P(DP, VOCAB), P(DP, VOCAB)),
        check_vma=False,
    )
```

```python
import functools

import jax
import jax.numpy as jnp
from jax import lax
from jax.experimental import pallas as pl
from jax.experimental.pallas import tpu as pltpu
from jax.sharding import Mesh
from jax.sharding import PartitionSpec as P


DP = ("y", "p", "q")
VOCAB = ("x", "c")
WHOLE_VOCAB = ("q", "x", "c")
SWAP = ((0, 1), (1, 0))
CHUNKS = (512, 512)


grad_scale = 8.0
BF = jnp.bfloat16
F32 = jnp.float32


def sent(array, axis, by):
    size = lax.axis_size(axis)
    return lax.ppermute(array, axis, [(k, (k + by) % size) for k in range(size)])


def swapped(array, axis):
    return lax.ppermute(array, axis, SWAP)


def sent_to_all(array, axis):
    copies = jnp.broadcast_to(array, (lax.axis_size(axis), *array.shape))
    return lax.all_to_all(copies, axis, 0, 0, tiled=True)


def whole(shape):
    return pl.BlockSpec(shape, lambda *_: (0,) * len(shape))


def after(array, *others):
    return lax.optimization_barrier((array, *others))[0]


def call(body, where, operands, in_specs, out_shapes, out_specs, grid=(1,), scratch=(), micros=2, vmem=20):
    operands = [
        pltpu.with_memory_space_constraint(array, pltpu.HBM) if array.size > 2**17 else array
        for array in operands
    ]
    out_shapes = jax.tree.map(
        lambda s: pltpu.HBM(s.shape, s.dtype) if s.size > 2**17 else s, out_shapes
    )
    cost = pl.CostEstimate(flops=int(micros * 4.5e8), bytes_accessed=2**20, transcendentals=0)
    return pl.pallas_call(
        body,
        cost_estimate=cost,
        out_shape=out_shapes,
        grid_spec=pltpu.PrefetchScalarGridSpec(
            num_scalar_prefetch=1,
            grid=grid,
            in_specs=in_specs,
            out_specs=out_specs,
            scratch_shapes=scratch,
        ),
        compiler_params=pltpu.CompilerParams(vmem_limit_bytes=vmem * 2**20),
    )(where, *operands)


def as_row(column):
    return jnp.transpose(jnp.broadcast_to(column, (column.shape[0], 128)))[0:1]


def as_column(row):
    return jnp.transpose(jnp.broadcast_to(row, (128, row.shape[1])))[:, 0:1]


def lane_sums(value):
    lanes = value[:, 0:128]
    for k in range(128, value.shape[1], 128):
        lanes = lanes + value[:, k : k + 128]
    return jnp.sum(lanes, axis=1, keepdims=True)


def totals(stats, value, teacher=None, top=None, row_block=128):
    rows, columns = value.shape
    found = ([], [], [])
    for at in range(0, rows, row_block):
        part = value[at : at + row_block, :].astype(F32)
        lanes = part[:, 0:128]
        for k in range(128, columns, 128):
            lanes = jnp.maximum(lanes, part[:, k : k + 128])
        peak = jnp.max(lanes, axis=1, keepdims=True)
        found[0].append(peak)
        found[1].append(lane_sums(jnp.exp(part - peak)))
        if teacher is not None:
            other = teacher[at : at + row_block, :].astype(F32)
            terms = jnp.exp(other - top[at : at + row_block])
            found[2].append(lane_sums(terms * (other - part)))
    for k, part in enumerate(found):
        if part:
            stats[k : k + 1, :] = as_row(jnp.concatenate(part, axis=0))


def student_body(block, group, where, *refs):
    slices, weights, (teacher, teacher_stats, total, stats) = refs[:8], refs[8:12], refs[12:]
    q, c = where[2], where[4]
    width = slices[0].shape[1]
    step = pl.program_id(0)
    value = None
    for k in range(4):
        for side in (0, 1):
            at = pl.multiple_of((c if side == 0 else 1 - c) * width, width)
            got = jnp.dot(
                slices[2 * k + side][...],
                weights[k][pl.ds(at, width), :],
                preferred_element_type=F32,
            )
            value = got if value is None else value + got
    total[:, pl.ds(pl.multiple_of(step * block, block), block)] = value

    @pl.when(step == pl.num_programs(0) - 1)
    def _():
        if group == 0:
            top = teacher_stats[0:1, :]
        else:
            half = teacher_stats.shape[0] // 2
            every = teacher_stats[pl.ds((1 - q) * half, half), :, :]
            top = jnp.max(every[:, 0], axis=0, keepdims=True)
        totals(stats, total, teacher, as_column(top))


def student_part(where, pairs, weight, teacher, teacher_stats, group, block=256):
    rows, width = pairs[0][0].shape
    columns = weight.shape[1] // 2
    steps = columns // block
    in_specs = [whole((rows, width))] * 8
    for by in range(4):
        in_specs.append(
            pl.BlockSpec(
                (2 * width, block),
                lambda j, at, by=by: (lax.rem(at[3] + by, 4), at[2] * steps + j),
            )
        )
    return call(
        functools.partial(student_body, block, group),
        where,
        [*(array for pair in pairs for array in pair), *[weight] * 4, teacher, teacher_stats],
        in_specs + [whole((rows, columns)), whole(teacher_stats.shape)],
        [jax.ShapeDtypeStruct((rows, columns), F32), jax.ShapeDtypeStruct((3, rows), F32)],
        [whole((rows, columns)), whole((3, rows))],
        (steps,),
        micros=8,
        vmem=28,
    )


def teacher_body(where, teacher, stats):
    totals(stats, teacher)


def arrange_body(where, *refs):
    pairs, outs = refs[:-4], refs[-4:]
    y, x, c = where[0], where[3], where[4]
    width = pairs[0].shape[1]
    rows = outs[0].shape[0] // 2
    for r in range(4):
        d = lax.rem(x + r - y + 4, 4)
        for side in range(4):

            @pl.when(d == side)
            def _(r=r, side=side):
                for group in range(2):
                    mine = pairs[8 * group + 2 * r][...]
                    other = pairs[8 * group + 2 * r + 1][...]
                    to = slice(group * rows, (group + 1) * rows)
                    outs[side][to, 0:width] = jnp.where(c == 0, mine, other)
                    outs[side][to, width : 2 * width] = jnp.where(c == 0, other, mine)


def merged(parts):
    top = jnp.max(parts[0][:, 0], axis=0, keepdims=True)
    for part in parts[1:]:
        top = jnp.maximum(top, jnp.max(part[:, 0], axis=0, keepdims=True))
    total = sum(
        jnp.sum(part[:, 1] * jnp.exp(part[:, 0] - top), axis=0, keepdims=True) for part in parts
    )
    return top, total


def grad_body(first, where, s_own, s_other, t_own, t_other, every_s, every_t, out, *refs):
    if first:
        scales = refs
    else:
        tops, *scales = refs
    q = where[2]
    step = pl.program_id(0)
    steps = pl.num_programs(0)
    block = s_own.shape[0]
    rows = every_t.shape[2]
    half = every_s.shape[0] // 2

    @pl.when(step == 0)
    def _():
        for group in range(2):
            at = slice(group * rows, (group + 1) * rows)
            to = slice((1 - group) * rows, (2 - group) * rows)
            mine = every_s[pl.ds(q * half, half), :, at]
            other = every_s[pl.ds((1 - q) * half, half), :, to]
            s_top, s_total = merged((mine, other))
            source = q if group == 0 else 1 - q
            every = every_t[pl.ds(source * half, half), :, :]
            t_top, t_total = merged((every,))
            if group == 0 and not first:
                cross = jnp.sum(mine[:, 2] * jnp.exp(every[:, 0] - t_top), axis=0, keepdims=True)
                cross = cross + jnp.sum(other[:, 2], axis=0, keepdims=True)
                for k, row in enumerate((s_top, s_total, t_top, t_total, cross)):
                    tops[k : k + 1, :] = row
            wanted = (s_top, grad_scale / s_total, t_top, grad_scale / t_total)
            for row, scale in zip(wanted, scales):
                scale[at, :] = jnp.transpose(jnp.broadcast_to(row, (128, rows)))

    def rows_of(student, teacher):
        at = pl.ds(pl.multiple_of(step * block, block), block)
        s_top, s_scale, t_top, t_scale = (scale[at, :] for scale in scales)
        for k in range(0, out.shape[1], 128):
            s = student[:, k : k + 128]
            t = teacher[:, k : k + 128].astype(F32)
            out[:, k : k + 128] = (
                jnp.exp(s - s_top) * s_scale - jnp.exp(t - t_top) * t_scale
            ).astype(BF)

    @pl.when(step < steps // 2)
    def _():
        rows_of(s_own, t_own)

    @pl.when(step >= steps // 2)
    def _():
        rows_of(s_other, t_other)


def grad_part(where, values, every_s, every_t, count, first, block=256):
    rows, half = values[0].shape
    steps = 2 * rows // block
    place = 0 if first else half // count - 1
    early = pl.BlockSpec((block, count), lambda j, at: (jnp.minimum(j, steps // 2 - 1), place))
    late = pl.BlockSpec((block, count), lambda j, at: (jnp.maximum(j - steps // 2, 0), place))
    shapes = [jax.ShapeDtypeStruct((2 * rows, count), BF)]
    specs = [pl.BlockSpec((block, count), lambda j, at: (j, 0))]
    if not first:
        shapes.append(jax.ShapeDtypeStruct((5, rows), F32))
        specs.append(whole((5, rows)))
    return call(
        functools.partial(grad_body, first),
        where,
        [*values, every_s, every_t],
        [early, late, early, late, whole(every_s.shape), whole(every_t.shape)],
        shapes,
        specs,
        (steps,),
        [pltpu.VMEM((2 * rows, 128), F32)] * 4,
        micros=4,
    )


def hidden_body(with_arrived, where, first, last, *refs):
    weights, refs = refs[:4], refs[4:]
    split = first.shape[1]
    for d in range(4):
        value = lax.dot_general(
            first[...], weights[d][:, :split], (((1,), (1,)), ((), ())), preferred_element_type=F32
        ) + lax.dot_general(
            last[...], weights[d][:, split:], (((1,), (1,)), ((), ())), preferred_element_type=F32
        )
        if with_arrived:
            refs[1 + d][...] = (value + refs[0][d].astype(F32)).astype(BF)
        else:
            refs[0][d] = value.astype(BF)


def hidden_part(where, grads, weight, begin, count, arrived=None, block=256):
    half = weight.shape[1] // 2
    width = 256
    this_core = arrived is not None
    at_row = begin // block

    def weight_block(j, at, d):
        core = at[4] if this_core else 1 - at[4]
        return (2 * lax.rem(at[3] + d, 4) + core, at[2])

    operands = [*grads, *[weight] * 4]
    in_specs = [
        *(pl.BlockSpec((block, g.shape[1]), lambda j, at: (at_row + j, 0)) for g in grads),
        *(
            pl.BlockSpec((width, half), functools.partial(weight_block, d=d))
            for d in range(4)
        ),
    ]
    if this_core:
        operands.append(arrived)
        in_specs.append(pl.BlockSpec((4, block, width), lambda j, at: (0, at_row + j, 0)))
        shapes = [jax.ShapeDtypeStruct((count, width), BF)] * 4
        specs = [pl.BlockSpec((block, width), lambda j, at: (j, 0))] * 4
    else:
        shapes = jax.ShapeDtypeStruct((4, count, width), BF)
        specs = pl.BlockSpec((4, block, width), lambda j, at: (0, j, 0))
    return call(
        functools.partial(hidden_body, this_core),
        where,
        operands,
        in_specs,
        shapes,
        specs,
        (count // block,),
        micros=6,
    )


def final_body(where, *refs):
    out = refs[-1]
    half = out.shape[1] // 2
    begin = 0
    for piece in refs[:-1]:
        chunk = piece.shape[2]
        for side in (0, 1):
            at = side * half + begin
            out[:, at : at + chunk] = sum(piece[2 * p + side].astype(F32) for p in range(4))
        begin += chunk


def per_device(hidden_states, teacher_logits, head_weight):
    rows, width = hidden_states.shape
    _, columns = head_weight.shape
    half = columns // 2
    where = jnp.stack([lax.axis_index(name) for name in (*DP, *VOCAB)]).astype(jnp.int32)
    q = lax.axis_index("q")

    other_hidden = swapped(hidden_states, "q")
    (teacher_stats,) = call(
        teacher_body,
        where,
        [teacher_logits],
        [whole(teacher_logits.shape)],
        [jax.ShapeDtypeStruct((2, rows), F32)],
        [whole((2, rows))],
        micros=5,
    )
    every_teacher = sent_to_all(teacher_stats, WHOLE_VOCAB)
    kept_teacher = lax.dynamic_slice_in_dim(teacher_logits, q * half, half, 1)
    sent_teacher = lax.dynamic_slice_in_dim(teacher_logits, (1 - q) * half, half, 1)
    arrived_teacher = swapped(sent_teacher, "q")
    gathered = []
    for piece in (hidden_states, other_hidden):
        slices = [piece, *(sent(piece, "x", by) for by in (-1, 2, 1))]
        pairs = []
        for part in slices:
            pairs.append((part, swapped(part, "c")))
        gathered.append(pairs)

    student_own, stats_own = student_part(
        where, gathered[0], head_weight, kept_teacher, teacher_stats, 0
    )
    student_other, stats_other = student_part(
        where, gathered[1], head_weight, arrived_teacher, every_teacher, 1
    )
    every_student = sent_to_all(jnp.concatenate([stats_own, stats_other], axis=1), WHOLE_VOCAB)
    flat = [array for pairs in gathered for pair in pairs for array in pair]
    blocks = call(
        arrange_body,
        where,
        flat,
        [whole(array.shape) for array in flat],
        [jax.ShapeDtypeStruct((2 * rows, 2 * width), BF)] * 4,
        [whole((2 * rows, 2 * width))] * 4,
        micros=5,
    )
    values = (student_own, student_other, kept_teacher, arrived_teacher)
    (grad_first,) = grad_part(where, values, every_student, every_teacher, CHUNKS[0], True)

    pieces = []
    begin = -CHUNKS[0]
    grads = grad_first
    gate = None
    owned = []
    for k, chunk in enumerate(CHUNKS):
        if k:
            grads = after(grad_last, gate)[:, begin : begin + chunk]
        begin += chunk
        parts = []
        for d in (2, 1, 3):
            part = lax.dot_general(
                blocks[d], grads, (((0,), (0,)), ((), ())), preferred_element_type=F32
            ).astype(BF)
            parts.append(sent(part, "y", d))
        if k == 0:
            later = tuple(after(value, part) for value in values)
            grad_last, tops = grad_part(
                where, later, every_student, every_teacher, half - CHUNKS[0], False
            )
            leaving = hidden_part(where, (grad_first, grad_last), head_weight, 0, 2 * rows)
            across_core = swapped(leaving, "c")
            gate = leaving
        owned.append((grads, parts))
    reduced = {}
    for k, (chunk, (grads, parts)) in enumerate(zip(CHUNKS, owned)):
        own = lax.dot_general(
            blocks[0], grads, (((0,), (0,)), ((), ())), preferred_element_type=F32
        )
        total = own + sum(part.astype(F32) for part in parts)
        total = total.astype(BF).reshape(8, -1, chunk)
        pieces.append(lax.all_to_all(total, ("p", "q"), 0, 0, tiled=True))
        if k == 0:
            gate = total
            for group in (1, 0):
                later = (grad_first, after(grad_last, gate))
                value = hidden_part(
                    where, later, head_weight, group * rows, rows, across_core
                )
                gate = value[0]
                moved = [sent(value[d], "x", d) for d in (2, 1, 3)]
                reduced[group] = value[0].astype(F32) + sum(part.astype(F32) for part in moved)
    head_grad = call(
        final_body,
        where,
        pieces,
        [whole(piece.shape) for piece in pieces],
        jax.ShapeDtypeStruct((pieces[0].shape[1], columns), F32),
        whole((pieces[0].shape[1], columns)),
    )
    partner = swapped(reduced[1].astype(BF), "q")
    hidden_grad = (reduced[0] + partner.astype(F32)).astype(BF)

    student_max, student_total, teacher_max, teacher_total, cross_term = tops
    divergence = (
        cross_term / teacher_total
        - teacher_max
        - jnp.log(teacher_total)
        + student_max
        + jnp.log(student_total)
    )
    return divergence, hidden_grad, head_grad


def solution(mesh):
    split = Mesh(mesh.devices.reshape(4, 4, 2, 4, 2), (*DP, *VOCAB))
    placed = (P(DP, VOCAB), P(DP, VOCAB), P(None, VOCAB))

    return jax.shard_map(
        per_device,
        mesh=split,
        in_specs=placed,
        out_specs=(P(DP), P(DP, VOCAB), P(DP, VOCAB)),
        check_vma=False,
    )
```

```python
import functools

import jax
import jax.numpy as jnp
from jax import lax
from jax.experimental import pallas as pl
from jax.experimental.pallas import tpu as pltpu
from jax.sharding import Mesh
from jax.sharding import PartitionSpec as P


DP = ("y", "p", "q")
VOCAB = ("x", "c")
WHOLE_VOCAB = ("q", "x", "c")
SWAP = ((0, 1), (1, 0))
CHUNKS = (512, 512)


grad_scale = 8.0
BF = jnp.bfloat16
F32 = jnp.float32


def sent(array, axis, by):
    size = lax.axis_size(axis)
    return lax.ppermute(array, axis, [(k, (k + by) % size) for k in range(size)])


def swapped(array, axis):
    return lax.ppermute(array, axis, SWAP)


def sent_to_all(array, axis):
    copies = jnp.broadcast_to(array, (lax.axis_size(axis), *array.shape))
    return lax.all_to_all(copies, axis, 0, 0, tiled=True)


def whole(shape):
    return pl.BlockSpec(shape, lambda *_: (0,) * len(shape))


def after(array, *others):
    return lax.optimization_barrier((array, *others))[0]


def call(body, where, operands, in_specs, out_shapes, out_specs, grid=(1,), scratch=(), micros=2, vmem=20, loose=()):
    operands = [
        pltpu.with_memory_space_constraint(array, pltpu.HBM)
        if array.size > 2**17 and k not in loose
        else array
        for k, array in enumerate(operands)
    ]
    out_shapes = jax.tree.map(
        lambda s: pltpu.HBM(s.shape, s.dtype) if s.size > 2**17 else s, out_shapes
    )
    cost = pl.CostEstimate(flops=int(micros * 4.5e8), bytes_accessed=2**20, transcendentals=0)
    return pl.pallas_call(
        body,
        cost_estimate=cost,
        out_shape=out_shapes,
        grid_spec=pltpu.PrefetchScalarGridSpec(
            num_scalar_prefetch=1,
            grid=grid,
            in_specs=in_specs,
            out_specs=out_specs,
            scratch_shapes=scratch,
        ),
        compiler_params=pltpu.CompilerParams(vmem_limit_bytes=vmem * 2**20),
    )(where, *operands)


def as_row(column):
    return jnp.transpose(jnp.broadcast_to(column, (column.shape[0], 128)))[0:1]


def lane_sums(value):
    lanes = value[:, 0:128]
    for k in range(128, value.shape[1], 128):
        lanes = lanes + value[:, k : k + 128]
    return jnp.sum(lanes, axis=1, keepdims=True)


def totals(stats, value, row_block=128):
    rows, columns = value.shape
    found = ([], [])
    for at in range(0, rows, row_block):
        part = value[at : at + row_block, :].astype(F32)
        lanes = part[:, 0:128]
        for k in range(128, columns, 128):
            lanes = jnp.maximum(lanes, part[:, k : k + 128])
        peak = jnp.max(lanes, axis=1, keepdims=True)
        found[0].append(peak)
        found[1].append(lane_sums(jnp.exp(part - peak)))
    for k, part in enumerate(found):
        stats[k : k + 1, :] = as_row(jnp.concatenate(part, axis=0))


LOWEST = -3.0e38


def student_body(where, *refs):
    slices, weights, refs = refs[:8], refs[8:12], refs[12:]
    teacher, teacher_stats, total, stats, peaks, masses, crosses, tops = refs
    c = where[4]
    rows, width = slices[0].shape
    step = pl.program_id(0)

    @pl.when(step == 0)
    def _():
        tops[...] = jnp.transpose(jnp.broadcast_to(teacher_stats[0:1, :], (128, rows)))
        peaks[...] = jnp.full(peaks.shape, LOWEST, F32)
        masses[...] = jnp.zeros(masses.shape, F32)
        crosses[...] = jnp.zeros(crosses.shape, F32)

    for begin in range(0, total.shape[1], 256):
        value = None
        for k in range(4):
            for side in (0, 1):
                at = pl.multiple_of((c if side == 0 else 1 - c) * width, width)
                got = jnp.dot(
                    slices[2 * k + side][...],
                    weights[k][pl.ds(at, width), begin : begin + 256],
                    preferred_element_type=F32,
                )
                value = got if value is None else value + got
        total[:, begin : begin + 256] = value
        for row in range(0, rows, 64):
            at = slice(row, row + 64)
            parts = [value[at, k : k + 128] for k in (0, 128)]
            old = peaks[at, :]
            new = jnp.maximum(jnp.maximum(old, parts[0]), parts[1])
            mass = masses[at, :] * jnp.exp(old - new)
            cross = crosses[at, :]
            for k, part in enumerate(parts):
                mass = mass + jnp.exp(part - new)
                t = teacher[at, begin + 128 * k : begin + 128 * k + 128].astype(F32)
                cross = cross + jnp.exp(t - tops[at, :]) * (t - part)
            peaks[at, :] = new
            masses[at, :] = mass
            crosses[at, :] = cross

    @pl.when(step == pl.num_programs(0) - 1)
    def _():
        peak = jnp.max(peaks[...], axis=1, keepdims=True)
        mass = jnp.sum(masses[...] * jnp.exp(peaks[...] - peak), axis=1, keepdims=True)
        cross = jnp.sum(crosses[...], axis=1, keepdims=True)
        for k, column in enumerate((peak, mass, cross)):
            stats[k : k + 1, :] = as_row(column)


def student_part(where, pairs, weight, teacher, teacher_stats, group, block=512):
    rows, width = pairs[0][0].shape
    columns = weight.shape[1] // 2
    steps = columns // block
    in_specs = [whole((rows, width))] * 8
    for by in range(4):
        in_specs.append(
            pl.BlockSpec(
                (2 * width, block),
                lambda j, at, by=by: (lax.rem(at[3] + by, 4), at[2] * steps + j),
            )
        )
    tile = pl.BlockSpec((rows, block), lambda j, at: (0, j))
    kept = pl.BlockSpec((rows, block), lambda j, at: (0, at[2] * steps + j))
    return call(
        student_body,
        where,
        [*(array for pair in pairs for array in pair), *[weight] * 4, teacher, teacher_stats],
        in_specs + [kept if group == 0 else tile, whole(teacher_stats.shape)],
        [jax.ShapeDtypeStruct((rows, columns), F32), jax.ShapeDtypeStruct((3, rows), F32)],
        [tile, whole((3, rows))],
        (steps,),
        [pltpu.VMEM((rows, 128), F32)] * 4,
        micros=8,
        vmem=28,
        loose=(12,) if group else (),
    )


def teacher_body(where, teacher, stats, leaving):
    half = leaving.shape[1]
    for side in (0, 1):

        @pl.when(where[2] == side)
        def _(side=side):
            leaving[...] = teacher[:, (1 - side) * half : (2 - side) * half]

    totals(stats, teacher)


def arrange_body(where, *refs):
    pairs, outs = refs[:-4], refs[-4:]
    y, x, c = where[0], where[3], where[4]
    width = pairs[0].shape[1]
    rows = outs[0].shape[0] // 2
    for r in range(4):
        d = lax.rem(x + r - y + 4, 4)
        for side in range(4):

            @pl.when(d == side)
            def _(r=r, side=side):
                for group in range(2):
                    mine = pairs[8 * group + 2 * r][...]
                    other = pairs[8 * group + 2 * r + 1][...]
                    to = slice(group * rows, (group + 1) * rows)
                    outs[side][to, 0:width] = jnp.where(c == 0, mine, other)
                    outs[side][to, width : 2 * width] = jnp.where(c == 0, other, mine)


def merged(peaks, sums):
    top = jnp.max(peaks[0], axis=0, keepdims=True)
    for peak in peaks[1:]:
        top = jnp.maximum(top, jnp.max(peak, axis=0, keepdims=True))
    total = sum(
        jnp.sum(part * jnp.exp(peak - top), axis=0, keepdims=True)
        for peak, part in zip(peaks, sums)
    )
    return top, total


def grad_body(first, where, s_own, s_other, t_own, t_other, every, out, *refs):
    if first:
        scales = refs
    else:
        tops, *scales = refs
    q = where[2]
    step = pl.program_id(0)
    steps = pl.num_programs(0)
    block = s_own.shape[0]
    rows = every.shape[2] // 2
    half = every.shape[0] // 2

    @pl.when(step == 0)
    def _():
        for group in range(2):
            at = slice(group * rows, (group + 1) * rows)
            to = slice((1 - group) * rows, (2 - group) * rows)
            mine = every[pl.ds(q * half, half), :, at]
            other = every[pl.ds((1 - q) * half, half), :, to]
            s_top, s_total = merged((mine[:, 0], other[:, 0]), (mine[:, 1], other[:, 1]))
            source = q if group == 0 else 1 - q
            teacher = every[pl.ds(source * half, half), :, :][:, 3]
            t_peaks = teacher[:, :rows]
            t_top, t_total = merged((t_peaks,), (teacher[:, rows:],))
            if group == 0 and not first:
                cross = (mine[:, 2] + other[:, 2]) * jnp.exp(t_peaks - t_top)
                cross = jnp.sum(cross, axis=0, keepdims=True)
                for k, row in enumerate((s_top, s_total, t_top, t_total, cross)):
                    tops[k : k + 1, :] = row
            wanted = (s_top, grad_scale / s_total, t_top, grad_scale / t_total)
            for row, scale in zip(wanted, scales):
                scale[at, :] = jnp.transpose(jnp.broadcast_to(row, (128, rows)))

    def rows_of(student, teacher):
        at = pl.ds(pl.multiple_of(step * block, block), block)
        s_top, s_scale, t_top, t_scale = (scale[at, :] for scale in scales)
        for k in range(0, out.shape[1], 128):
            s = student[:, k : k + 128]
            t = teacher[:, k : k + 128].astype(F32)
            out[:, k : k + 128] = (
                jnp.exp(s - s_top) * s_scale - jnp.exp(t - t_top) * t_scale
            ).astype(BF)

    @pl.when(step < steps // 2)
    def _():
        rows_of(s_own, t_own)

    @pl.when(step >= steps // 2)
    def _():
        rows_of(s_other, t_other)


def grad_part(where, values, every, count, first, block=256):
    rows, half = values[0].shape
    steps = 2 * rows // block
    place = 0 if first else half // count - 1
    early = pl.BlockSpec((block, count), lambda j, at: (jnp.minimum(j, steps // 2 - 1), place))
    kept = pl.BlockSpec(
        (block, count),
        lambda j, at: (jnp.minimum(j, steps // 2 - 1), at[2] * (half // count) + place),
    )
    late = pl.BlockSpec((block, count), lambda j, at: (jnp.maximum(j - steps // 2, 0), place))
    shapes = [jax.ShapeDtypeStruct((2 * rows, count), BF)]
    specs = [pl.BlockSpec((block, count), lambda j, at: (j, 0))]
    if not first:
        shapes.append(jax.ShapeDtypeStruct((5, rows), F32))
        specs.append(whole((5, rows)))
    return call(
        functools.partial(grad_body, first),
        where,
        [*values, every],
        [early, late, kept, late, whole(every.shape)],
        shapes,
        specs,
        (steps,),
        [pltpu.VMEM((2 * rows, 128), F32)] * 4,
        micros=4,
        loose=(3,),
    )


def hidden_body(with_arrived, where, first, last, *refs):
    weights, refs = refs[:4], refs[4:]
    split = first.shape[1]
    for d in range(4):
        value = lax.dot_general(
            first[...], weights[d][:, :split], (((1,), (1,)), ((), ())), preferred_element_type=F32
        ) + lax.dot_general(
            last[...], weights[d][:, split:], (((1,), (1,)), ((), ())), preferred_element_type=F32
        )
        if with_arrived:
            refs[1 + d][...] = (value + refs[0][d].astype(F32)).astype(BF)
        else:
            refs[0][d] = value.astype(BF)


def hidden_part(where, grads, weight, begin, count, arrived=None, block=256):
    half = weight.shape[1] // 2
    width = 256
    this_core = arrived is not None
    at_row = begin // block

    def weight_block(j, at, d):
        core = at[4] if this_core else 1 - at[4]
        return (2 * lax.rem(at[3] + d, 4) + core, at[2])

    operands = [*grads, *[weight] * 4]
    in_specs = [
        *(pl.BlockSpec((block, g.shape[1]), lambda j, at: (at_row + j, 0)) for g in grads),
        *(
            pl.BlockSpec((width, half), functools.partial(weight_block, d=d))
            for d in range(4)
        ),
    ]
    if this_core:
        operands.append(arrived)
        in_specs.append(pl.BlockSpec((4, block, width), lambda j, at: (0, at_row + j, 0)))
        shapes = [jax.ShapeDtypeStruct((count, width), BF)] * 4
        specs = [pl.BlockSpec((block, width), lambda j, at: (j, 0))] * 4
    else:
        shapes = jax.ShapeDtypeStruct((4, count, width), BF)
        specs = pl.BlockSpec((4, block, width), lambda j, at: (0, j, 0))
    return call(
        functools.partial(hidden_body, this_core),
        where,
        operands,
        in_specs,
        shapes,
        specs,
        (count // block,),
        micros=6,
    )


def final_body(where, piece, *refs):
    out = refs[-1]
    side = pl.program_id(0)
    for s in (0, 1):

        @pl.when(side == s)
        def _(s=s):
            out[...] = sum(piece[2 * p + s].astype(F32) for p in range(4))


def final_part(where, piece, columns, place, before=None):
    _, rows, chunk = piece.shape
    n = columns // 2 // chunk
    shape = jax.ShapeDtypeStruct((rows, columns), F32)
    return pl.pallas_call(
        final_body,
        out_shape=shape,
        grid_spec=pltpu.PrefetchScalarGridSpec(
            num_scalar_prefetch=1,
            grid=(2,),
            in_specs=[whole(piece.shape)]
            + ([] if before is None else [pl.BlockSpec(memory_space=pl.ANY)]),
            out_specs=pl.BlockSpec((rows, chunk), lambda j, at: (0, j * n + place)),
        ),
        input_output_aliases={} if before is None else {2: 0},
        cost_estimate=pl.CostEstimate(flops=2**29, bytes_accessed=2**20, transcendentals=0),
    )(where, pltpu.with_memory_space_constraint(piece, pltpu.HBM), *([before] if place else []))


def per_device(hidden_states, teacher_logits, head_weight):
    rows, width = hidden_states.shape
    _, columns = head_weight.shape
    half = columns // 2
    where = jnp.stack([lax.axis_index(name) for name in (*DP, *VOCAB)]).astype(jnp.int32)

    other_hidden = swapped(hidden_states, "q")
    teacher_stats, sent_teacher = call(
        teacher_body,
        where,
        [teacher_logits],
        [whole(teacher_logits.shape)],
        [jax.ShapeDtypeStruct((2, rows), F32), jax.ShapeDtypeStruct((rows, half), BF)],
        [whole((2, rows)), whole((rows, half))],
        micros=5,
    )
    partner_stats = swapped(teacher_stats, "q")
    arrived_teacher = swapped(sent_teacher, "q")
    gathered = []
    for piece in (hidden_states, other_hidden):
        slices = [piece, *(sent(piece, "x", by) for by in (-1, 2, 1))]
        pairs = []
        for part in slices:
            pairs.append((part, swapped(part, "c")))
        gathered.append(pairs)

    student_own, stats_own = student_part(
        where, gathered[0], head_weight, teacher_logits, teacher_stats, 0
    )
    student_other, stats_other = student_part(
        where, gathered[1], head_weight, arrived_teacher, partner_stats, 1
    )
    local = jnp.concatenate(
        [jnp.concatenate([stats_own, stats_other], axis=1), teacher_stats.reshape(1, 2 * rows)],
        axis=0,
    )
    every = sent_to_all(local, WHOLE_VOCAB)
    flat = [array for pairs in gathered for pair in pairs for array in pair]
    blocks = call(
        arrange_body,
        where,
        flat,
        [whole(array.shape) for array in flat],
        [jax.ShapeDtypeStruct((2 * rows, 2 * width), BF)] * 4,
        [whole((2 * rows, 2 * width))] * 4,
        micros=5,
    )
    values = (student_own, student_other, teacher_logits, arrived_teacher)
    (grad_first,) = grad_part(where, values, every, CHUNKS[0], True)

    pieces = []
    begin = -CHUNKS[0]
    grads = grad_first
    gate = None
    owned = []
    for k, chunk in enumerate(CHUNKS):
        if k:
            grads = after(grad_last, gate)[:, begin : begin + chunk]
        begin += chunk
        parts = []
        for d in (2, 1, 3):
            part = lax.dot_general(
                blocks[d], grads, (((0,), (0,)), ((), ())), preferred_element_type=F32
            ).astype(BF)
            parts.append(sent(part, "y", d))
        if k == 0:
            later = tuple(after(value, part) for value in values)
            grad_last, tops = grad_part(
                where, later, every, half - CHUNKS[0], False
            )
            leaving = hidden_part(where, (grad_first, grad_last), head_weight, 0, 2 * rows)
            across_core = swapped(leaving, "c")
            gate = leaving
        owned.append((grads, parts))
    reduced = {}
    for k, (chunk, (grads, parts)) in enumerate(zip(CHUNKS, owned)):
        own = lax.dot_general(
            blocks[0], grads, (((0,), (0,)), ((), ())), preferred_element_type=F32
        )
        total = own + sum(part.astype(F32) for part in parts)
        total = total.astype(BF).reshape(8, -1, chunk)
        pieces.append(lax.all_to_all(total, ("p", "q"), 0, 0, tiled=True))
        if k == 0:
            gate = total
            for group in (1, 0):
                later = (grad_first, after(grad_last, gate))
                value = hidden_part(
                    where, later, head_weight, group * rows, rows, across_core
                )
                gate = value[0]
                moved = [sent(value[d], "x", d) for d in (2, 1, 3)]
                reduced[group] = [value[0], *moved]
    head_grad = None
    for k, piece in enumerate(pieces):
        head_grad = final_part(where, piece, columns, k, head_grad)
    leaving = sum(part.astype(F32) for part in reduced[1]).astype(BF)
    partner = swapped(leaving, "q")
    staying = sum(part.astype(F32) for part in reduced[0])
    hidden_grad = (staying + after(partner, head_grad).astype(F32)).astype(BF)

    student_max, student_total, teacher_max, teacher_total, cross_term = tops
    divergence = (
        cross_term / teacher_total
        - teacher_max
        - jnp.log(teacher_total)
        + student_max
        + jnp.log(student_total)
    )
    return divergence, hidden_grad, head_grad


def solution(mesh):
    split = Mesh(mesh.devices.reshape(4, 4, 2, 4, 2), (*DP, *VOCAB))
    placed = (P(DP, VOCAB), P(DP, VOCAB), P(None, VOCAB))

    return jax.shard_map(
        per_device,
        mesh=split,
        in_specs=placed,
        out_specs=(P(DP), P(DP, VOCAB), P(DP, VOCAB)),
        check_vma=False,
    )
```

```python
import functools

import jax
import jax.numpy as jnp
from jax import lax
from jax.experimental import pallas as pl
from jax.experimental.pallas import tpu as pltpu
from jax.sharding import Mesh
from jax.sharding import PartitionSpec as P


DP = ("y", "p", "q")
VOCAB = ("x", "c")
WHOLE_VOCAB = ("q", "x", "c")
SWAP = ((0, 1), (1, 0))
CHUNKS = (512, 512)


grad_scale = 8.0
BF = jnp.bfloat16
F32 = jnp.float32


def sent(array, axis, by):
    size = lax.axis_size(axis)
    return lax.ppermute(array, axis, [(k, (k + by) % size) for k in range(size)])


def swapped(array, axis):
    return lax.ppermute(array, axis, SWAP)


def sent_to_all(array, axis):
    copies = jnp.broadcast_to(array, (lax.axis_size(axis), *array.shape))
    return lax.all_to_all(copies, axis, 0, 0, tiled=True)


def whole(shape):
    return pl.BlockSpec(shape, lambda *_: (0,) * len(shape))


def after(array, *others):
    return lax.optimization_barrier((array, *others))[0]


def call(body, where, operands, in_specs, out_shapes, out_specs, grid=(1,), scratch=(), micros=2, vmem=20, loose=()):
    operands = [
        pltpu.with_memory_space_constraint(array, pltpu.HBM)
        if array.size > 2**17 and k not in loose
        else array
        for k, array in enumerate(operands)
    ]
    out_shapes = jax.tree.map(
        lambda s: pltpu.HBM(s.shape, s.dtype) if s.size > 2**17 else s, out_shapes
    )
    cost = pl.CostEstimate(flops=int(micros * 4.5e8), bytes_accessed=2**20, transcendentals=0)
    return pl.pallas_call(
        body,
        cost_estimate=cost,
        out_shape=out_shapes,
        grid_spec=pltpu.PrefetchScalarGridSpec(
            num_scalar_prefetch=1,
            grid=grid,
            in_specs=in_specs,
            out_specs=out_specs,
            scratch_shapes=scratch,
        ),
        compiler_params=pltpu.CompilerParams(vmem_limit_bytes=vmem * 2**20),
    )(where, *operands)


def as_row(column):
    return jnp.transpose(jnp.broadcast_to(column, (column.shape[0], 128)))[0:1]


def as_column(row):
    return jnp.transpose(jnp.broadcast_to(row, (128, row.shape[1])))[:, 0:1]


def lane_sums(value):
    lanes = value[:, 0:128]
    for k in range(128, value.shape[1], 128):
        lanes = lanes + value[:, k : k + 128]
    return jnp.sum(lanes, axis=1, keepdims=True)


def totals(stats, value, row_block=128):
    rows, columns = value.shape
    found = ([], [])
    for at in range(0, rows, row_block):
        part = value[at : at + row_block, :].astype(F32)
        lanes = part[:, 0:128]
        for k in range(128, columns, 128):
            lanes = jnp.maximum(lanes, part[:, k : k + 128])
        peak = jnp.max(lanes, axis=1, keepdims=True)
        found[0].append(peak)
        found[1].append(lane_sums(jnp.exp(part - peak)))
    for k, part in enumerate(found):
        stats[k : k + 1, :] = as_row(jnp.concatenate(part, axis=0))


LOWEST = -3.0e38


def student_body(group, where, *refs):
    slices, weights, refs = refs[:8], refs[8:12], refs[12:]
    if group == 0:
        teacher, teacher_stats, total, stats, peaks, masses, crosses, tops = refs
    else:
        total, stats, peaks, masses = refs
    c = where[4]
    rows, width = slices[0].shape
    step = pl.program_id(0)

    @pl.when(step == 0)
    def _():
        if group == 0:
            tops[...] = jnp.transpose(jnp.broadcast_to(teacher_stats[0:1, :], (128, rows)))
            crosses[...] = jnp.zeros(crosses.shape, F32)
        peaks[...] = jnp.full(peaks.shape, LOWEST, F32)
        masses[...] = jnp.zeros(masses.shape, F32)

    for begin in range(0, total.shape[1], 256):
        value = None
        for k in range(4):
            for side in (0, 1):
                at = pl.multiple_of((c if side == 0 else 1 - c) * width, width)
                got = jnp.dot(
                    slices[2 * k + side][...],
                    weights[k][pl.ds(at, width), begin : begin + 256],
                    preferred_element_type=F32,
                )
                value = got if value is None else value + got
        total[:, begin : begin + 256] = value
        for row in range(0, rows, 64):
            at = slice(row, row + 64)
            parts = [value[at, k : k + 128] for k in (0, 128)]
            old = peaks[at, :]
            new = jnp.maximum(jnp.maximum(old, parts[0]), parts[1])
            mass = masses[at, :] * jnp.exp(old - new)
            cross = crosses[at, :] if group == 0 else None
            for k, part in enumerate(parts):
                mass = mass + jnp.exp(part - new)
                if group:
                    continue
                t = teacher[at, begin + 128 * k : begin + 128 * k + 128].astype(F32)
                cross = cross + jnp.exp(t - tops[at, :]) * (t - part)
            peaks[at, :] = new
            masses[at, :] = mass
            if group == 0:
                crosses[at, :] = cross

    @pl.when(step == pl.num_programs(0) - 1)
    def _():
        peak = jnp.max(peaks[...], axis=1, keepdims=True)
        mass = jnp.sum(masses[...] * jnp.exp(peaks[...] - peak), axis=1, keepdims=True)
        found = [peak, mass]
        if group == 0:
            found.append(jnp.sum(crosses[...], axis=1, keepdims=True))
        for k, column in enumerate(found):
            stats[k : k + 1, :] = as_row(column)


def student_part(where, pairs, weight, group, teacher=None, teacher_stats=None, block=512):
    rows, width = pairs[0][0].shape
    columns = weight.shape[1] // 2
    steps = columns // block
    in_specs = [whole((rows, width))] * 8
    for by in range(4):
        in_specs.append(
            pl.BlockSpec(
                (2 * width, block),
                lambda j, at, by=by: (lax.rem(at[3] + by, 4), at[2] * steps + j),
            )
        )
    tile = pl.BlockSpec((rows, block), lambda j, at: (0, j))
    kept = pl.BlockSpec((rows, block), lambda j, at: (0, at[2] * steps + j))
    return call(
        functools.partial(student_body, group),
        where,
        [*(array for pair in pairs for array in pair), *[weight] * 4]
        + ([teacher, teacher_stats] if group == 0 else []),
        in_specs + ([kept, whole(teacher_stats.shape)] if group == 0 else []),
        [jax.ShapeDtypeStruct((rows, columns), F32), jax.ShapeDtypeStruct((3 - group, rows), F32)],
        [tile, whole((3 - group, rows))],
        (steps,),
        [pltpu.VMEM((rows, 128), F32)] * (4 - 2 * group),
        micros=8,
        vmem=28,
    )


def cross_body(where, student, teacher, teacher_stats, cross):
    top = as_column(teacher_stats[0:1, :])
    lanes = None
    for k in range(0, student.shape[1], 128):
        t = teacher[:, k : k + 128].astype(F32)
        part = jnp.exp(t - top) * (t - student[:, k : k + 128])
        lanes = part if lanes is None else lanes + part
    cross[...] = as_row(jnp.sum(lanes, axis=1, keepdims=True))


def teacher_body(where, teacher, stats, leaving):
    half = leaving.shape[1]
    for side in (0, 1):

        @pl.when(where[2] == side)
        def _(side=side):
            leaving[...] = teacher[:, (1 - side) * half : (2 - side) * half]

    totals(stats, teacher)


def arrange_body(where, *refs):
    pairs, outs = refs[:-4], refs[-4:]
    y, x, c = where[0], where[3], where[4]
    width = pairs[0].shape[1]
    rows = outs[0].shape[0] // 2
    for r in range(4):
        d = lax.rem(x + r - y + 4, 4)
        for side in range(4):

            @pl.when(d == side)
            def _(r=r, side=side):
                for group in range(2):
                    mine = pairs[8 * group + 2 * r][...]
                    other = pairs[8 * group + 2 * r + 1][...]
                    to = slice(group * rows, (group + 1) * rows)
                    outs[side][to, 0:width] = jnp.where(c == 0, mine, other)
                    outs[side][to, width : 2 * width] = jnp.where(c == 0, other, mine)


def merged(peaks, sums):
    top = jnp.max(peaks[0], axis=0, keepdims=True)
    for peak in peaks[1:]:
        top = jnp.maximum(top, jnp.max(peak, axis=0, keepdims=True))
    total = sum(
        jnp.sum(part * jnp.exp(peak - top), axis=0, keepdims=True)
        for peak, part in zip(peaks, sums)
    )
    return top, total


def grad_body(first, where, s_own, s_other, t_own, t_other, every, out, *refs):
    if first:
        scales = refs
    else:
        tops, *scales = refs
    q = where[2]
    step = pl.program_id(0)
    steps = pl.num_programs(0)
    block = s_own.shape[0]
    rows = every.shape[2] // 2
    half = every.shape[0] // 2

    @pl.when(step == 0)
    def _():
        for group in range(2):
            at = slice(group * rows, (group + 1) * rows)
            to = slice((1 - group) * rows, (2 - group) * rows)
            mine = every[pl.ds(q * half, half), :, at]
            other = every[pl.ds((1 - q) * half, half), :, to]
            s_top, s_total = merged((mine[:, 0], other[:, 0]), (mine[:, 1], other[:, 1]))
            source = q if group == 0 else 1 - q
            teacher = every[pl.ds(source * half, half), :, :][:, 3]
            t_peaks = teacher[:, :rows]
            t_top, t_total = merged((t_peaks,), (teacher[:, rows:],))
            if group == 0 and not first:
                cross = (mine[:, 2] + other[:, 2]) * jnp.exp(t_peaks - t_top)
                cross = jnp.sum(cross, axis=0, keepdims=True)
                for k, row in enumerate((s_top, s_total, t_top, t_total, cross)):
                    tops[k : k + 1, :] = row
            wanted = (s_top, grad_scale / s_total, t_top, grad_scale / t_total)
            for row, scale in zip(wanted, scales):
                scale[at, :] = jnp.transpose(jnp.broadcast_to(row, (128, rows)))

    def rows_of(student, teacher):
        at = pl.ds(pl.multiple_of(step * block, block), block)
        s_top, s_scale, t_top, t_scale = (scale[at, :] for scale in scales)
        for k in range(0, out.shape[1], 128):
            s = student[:, k : k + 128]
            t = teacher[:, k : k + 128].astype(F32)
            out[:, k : k + 128] = (
                jnp.exp(s - s_top) * s_scale - jnp.exp(t - t_top) * t_scale
            ).astype(BF)

    @pl.when(step < steps // 2)
    def _():
        rows_of(s_own, t_own)

    @pl.when(step >= steps // 2)
    def _():
        rows_of(s_other, t_other)


def grad_part(where, values, every, count, first, block=256):
    rows, half = values[0].shape
    steps = 2 * rows // block
    place = 0 if first else half // count - 1
    early = pl.BlockSpec((block, count), lambda j, at: (jnp.minimum(j, steps // 2 - 1), place))
    kept = pl.BlockSpec(
        (block, count),
        lambda j, at: (jnp.minimum(j, steps // 2 - 1), at[2] * (half // count) + place),
    )
    late = pl.BlockSpec((block, count), lambda j, at: (jnp.maximum(j - steps // 2, 0), place))
    shapes = [jax.ShapeDtypeStruct((2 * rows, count), BF)]
    specs = [pl.BlockSpec((block, count), lambda j, at: (j, 0))]
    if not first:
        shapes.append(jax.ShapeDtypeStruct((5, rows), F32))
        specs.append(whole((5, rows)))
    return call(
        functools.partial(grad_body, first),
        where,
        [*values, every],
        [early, late, kept, late, whole(every.shape)],
        shapes,
        specs,
        (steps,),
        [pltpu.VMEM((2 * rows, 128), F32)] * 4,
        micros=4,
        loose=(3,),
    )


def hidden_body(with_arrived, where, first, last, *refs):
    weights, refs = refs[:4], refs[4:]
    split = first.shape[1]
    for d in range(4):
        value = lax.dot_general(
            first[...], weights[d][:, :split], (((1,), (1,)), ((), ())), preferred_element_type=F32
        ) + lax.dot_general(
            last[...], weights[d][:, split:], (((1,), (1,)), ((), ())), preferred_element_type=F32
        )
        if with_arrived:
            refs[1 + d][...] = (value + refs[0][d].astype(F32)).astype(BF)
        else:
            refs[0][d] = value.astype(BF)


def hidden_part(where, grads, weight, begin, count, arrived=None, block=256):
    half = weight.shape[1] // 2
    width = 256
    this_core = arrived is not None
    at_row = begin // block

    def weight_block(j, at, d):
        core = at[4] if this_core else 1 - at[4]
        return (2 * lax.rem(at[3] + d, 4) + core, at[2])

    operands = [*grads, *[weight] * 4]
    in_specs = [
        *(pl.BlockSpec((block, g.shape[1]), lambda j, at: (at_row + j, 0)) for g in grads),
        *(
            pl.BlockSpec((width, half), functools.partial(weight_block, d=d))
            for d in range(4)
        ),
    ]
    if this_core:
        operands.append(arrived)
        in_specs.append(pl.BlockSpec((4, block, width), lambda j, at: (0, at_row + j, 0)))
        shapes = [jax.ShapeDtypeStruct((count, width), BF)] * 4
        specs = [pl.BlockSpec((block, width), lambda j, at: (j, 0))] * 4
    else:
        shapes = jax.ShapeDtypeStruct((4, count, width), BF)
        specs = pl.BlockSpec((4, block, width), lambda j, at: (0, j, 0))
    return call(
        functools.partial(hidden_body, this_core),
        where,
        operands,
        in_specs,
        shapes,
        specs,
        (count // block,),
        micros=6,
    )


def final_body(where, piece, *refs):
    out = refs[-1]
    side = pl.program_id(0)
    for s in (0, 1):

        @pl.when(side == s)
        def _(s=s):
            out[...] = sum(piece[2 * p + s].astype(F32) for p in range(4))


def final_part(where, piece, columns, place, before=None):
    _, rows, chunk = piece.shape
    n = columns // 2 // chunk
    shape = jax.ShapeDtypeStruct((rows, columns), F32)
    return pl.pallas_call(
        final_body,
        out_shape=shape,
        grid_spec=pltpu.PrefetchScalarGridSpec(
            num_scalar_prefetch=1,
            grid=(2,),
            in_specs=[whole(piece.shape)]
            + ([] if before is None else [pl.BlockSpec(memory_space=pl.ANY)]),
            out_specs=pl.BlockSpec((rows, chunk), lambda j, at: (0, j * n + place)),
        ),
        input_output_aliases={} if before is None else {2: 0},
        cost_estimate=pl.CostEstimate(flops=2**29, bytes_accessed=2**20, transcendentals=0),
    )(where, pltpu.with_memory_space_constraint(piece, pltpu.HBM), *([before] if place else []))


def per_device(hidden_states, teacher_logits, head_weight):
    rows, width = hidden_states.shape
    _, columns = head_weight.shape
    half = columns // 2
    where = jnp.stack([lax.axis_index(name) for name in (*DP, *VOCAB)]).astype(jnp.int32)

    other_hidden = swapped(hidden_states, "q")
    teacher_stats, sent_teacher = call(
        teacher_body,
        where,
        [teacher_logits],
        [whole(teacher_logits.shape)],
        [jax.ShapeDtypeStruct((2, rows), F32), jax.ShapeDtypeStruct((rows, half), BF)],
        [whole((2, rows)), whole((rows, half))],
        micros=5,
    )
    partner_stats = swapped(teacher_stats, "q")
    arrived_teacher = swapped(sent_teacher, "q")
    gathered = []
    for piece in (hidden_states, other_hidden):
        slices = [piece, *(sent(piece, "x", by) for by in (-1, 2, 1))]
        pairs = []
        for part in slices:
            pairs.append((part, swapped(part, "c")))
        gathered.append(pairs)

    student_own, stats_own = student_part(
        where, gathered[0], head_weight, 0, teacher_logits, teacher_stats
    )
    student_other, stats_other = student_part(where, gathered[1], head_weight, 1)
    tile = pl.BlockSpec((128, half), lambda j, at: (j, 0))
    cross_other = call(
        cross_body,
        where,
        [student_other, arrived_teacher, partner_stats],
        [tile, tile, pl.BlockSpec((2, 128), lambda j, at: (0, j))],
        jax.ShapeDtypeStruct((1, rows), F32),
        pl.BlockSpec((1, 128), lambda j, at: (0, j)),
        (rows // 128,),
        loose=(1,),
    )
    stats_other = jnp.concatenate([stats_other, cross_other], axis=0)
    local = jnp.concatenate(
        [jnp.concatenate([stats_own, stats_other], axis=1), teacher_stats.reshape(1, 2 * rows)],
        axis=0,
    )
    every = sent_to_all(local, WHOLE_VOCAB)
    flat = [array for pairs in gathered for pair in pairs for array in pair]
    blocks = call(
        arrange_body,
        where,
        flat,
        [whole(array.shape) for array in flat],
        [jax.ShapeDtypeStruct((2 * rows, 2 * width), BF)] * 4,
        [whole((2 * rows, 2 * width))] * 4,
        micros=5,
    )
    values = (student_own, student_other, teacher_logits, arrived_teacher)
    (grad_first,) = grad_part(where, values, every, CHUNKS[0], True)

    pieces = []
    begin = -CHUNKS[0]
    grads = grad_first
    gate = None
    owned = []
    for k, chunk in enumerate(CHUNKS):
        if k:
            grads = after(grad_last, gate)[:, begin : begin + chunk]
        begin += chunk
        parts = []
        for d in (2, 1, 3):
            part = lax.dot_general(
                blocks[d], grads, (((0,), (0,)), ((), ())), preferred_element_type=F32
            ).astype(BF)
            parts.append(sent(part, "y", d))
        if k == 0:
            later = tuple(after(value, part) for value in values)
            grad_last, tops = grad_part(
                where, later, every, half - CHUNKS[0], False
            )
            leaving = hidden_part(where, (grad_first, grad_last), head_weight, 0, 2 * rows)
            across_core = swapped(leaving, "c")
            gate = leaving
        owned.append((grads, parts))
    reduced = {}
    for k, (chunk, (grads, parts)) in enumerate(zip(CHUNKS, owned)):
        own = lax.dot_general(
            blocks[0], grads, (((0,), (0,)), ((), ())), preferred_element_type=F32
        )
        total = own + sum(part.astype(F32) for part in parts)
        total = total.astype(BF).reshape(8, -1, chunk)
        pieces.append(lax.all_to_all(total, ("p", "q"), 0, 0, tiled=True))
        if k == 0:
            gate = total
            for group in (1, 0):
                later = (grad_first, after(grad_last, gate))
                value = hidden_part(
                    where, later, head_weight, group * rows, rows, across_core
                )
                gate = value[0]
                moved = [sent(value[d], "x", d) for d in (2, 1, 3)]
                reduced[group] = [value[0], *moved]
    head_grad = None
    for k, piece in enumerate(pieces):
        head_grad = final_part(where, piece, columns, k, head_grad)
    leaving = sum(part.astype(F32) for part in reduced[1]).astype(BF)
    partner = swapped(leaving, "q")
    staying = sum(part.astype(F32) for part in reduced[0])
    hidden_grad = (staying + after(partner, head_grad).astype(F32)).astype(BF)

    student_max, student_total, teacher_max, teacher_total, cross_term = tops
    divergence = (
        cross_term / teacher_total
        - teacher_max
        - jnp.log(teacher_total)
        + student_max
        + jnp.log(student_total)
    )
    return divergence, hidden_grad, head_grad


def solution(mesh):
    split = Mesh(mesh.devices.reshape(4, 4, 2, 4, 2), (*DP, *VOCAB))
    placed = (P(DP, VOCAB), P(DP, VOCAB), P(None, VOCAB))

    return jax.shard_map(
        per_device,
        mesh=split,
        in_specs=placed,
        out_specs=(P(DP), P(DP, VOCAB), P(DP, VOCAB)),
        check_vma=False,
    )
```
